8 devices in a mesh: dp: 1 (over z), cz: 2 (over y), cy: 2 (over x), cx: 2 (over core).
Axes of the slice: x: 2, y: 2, z: 1, core: 2. Of those that a mesh axis runs over, the one named last changes fastest.
Arguments:
- x_act: bfloat16 [8192, 3072], P(('dp', 'cx', 'cz'), 'cy')
- w_up: bfloat16 [3072, 8192], P('cy', ('cz', 'cx'))
- w_down: bfloat16 [8192, 3072], P('cz', ('cy', 'cx'))
- z_grad: bfloat16 [8192, 3072], P(('dp', 'cx', 'cz'), 'cy')
Outputs:
- output 1: bfloat16 [8192, 3072], P(('dp', 'cx', 'cz'), 'cy')
- output 2: bfloat16 [3072, 8192], P(('dp', 'cy'), ('cz', 'cx'))
- output 3: bfloat16 [8192, 3072], P(('dp', 'cz'), ('cy', 'cx'))
All inputs are finite; a program needn't handle non-finite values.
Results may differ from the reference program's by a relative error of at most 0.0114789.
Values are sent between devices in bfloat16 or wider.
A program may use at most 1 GiB of HBM per device.

```python
import math
import jax
import jax.numpy as jnp

TOKENS = 8192
MODEL_DIM = 3072
HIDDEN_DIM = 8192
GELU_COEF = 0.044715
SQRT_TWO_PI = math.sqrt(2.0 / math.pi)


def gelu_parts(pre_act):
    inner_arg = SQRT_TWO_PI * (pre_act + GELU_COEF * pre_act * pre_act * pre_act)
    tanh_val = jnp.tanh(inner_arg)
    gelu_val = 0.5 * pre_act * (1.0 + tanh_val)
    gelu_slope = 0.5 * (1.0 + tanh_val) + 0.5 * pre_act * (1.0 - tanh_val * tanh_val) * SQRT_TWO_PI * (1.0 + 3.0 * GELU_COEF * pre_act * pre_act)
    return gelu_val, gelu_slope


def setup_inputs(seed: int = 0, part: int = 0) -> dict:
    base_key = jax.random.key(seed)
    key_up, key_down, key_acts = jax.random.split(base_key, 3)
    part_key = jax.random.fold_in(key_acts, part)
    key_x, key_z = jax.random.split(part_key)
    x_act = jax.random.normal(key_x, (TOKENS, MODEL_DIM), jnp.float32)
    w_up = jax.random.normal(key_up, (MODEL_DIM, HIDDEN_DIM), jnp.float32) * MODEL_DIM ** -0.5
    w_down = jax.random.normal(key_down, (HIDDEN_DIM, MODEL_DIM), jnp.float32) * HIDDEN_DIM ** -0.5
    z_grad = jax.random.normal(key_z, (TOKENS, MODEL_DIM), jnp.float32)
    return {"x_act": x_act.astype(jnp.bfloat16), "w_up": w_up.astype(jnp.bfloat16), "w_down": w_down.astype(jnp.bfloat16), "z_grad": z_grad.astype(jnp.bfloat16)}


def reference(x_act, w_up, w_down, z_grad):
    pre_act = jnp.dot(x_act, w_up, preferred_element_type=jnp.float32).astype(jnp.bfloat16).astype(jnp.float32)
    gelu_val, gelu_slope = gelu_parts(pre_act)
    hidden = gelu_val.astype(jnp.bfloat16)
    h_grad = jnp.dot(z_grad, w_down.T, preferred_element_type=jnp.float32)
    pre_grad = (h_grad * gelu_slope).astype(jnp.bfloat16)
    x_grad = jnp.dot(pre_grad, w_up.T, preferred_element_type=jnp.float32).astype(jnp.bfloat16)
    up_grad = jnp.dot(x_act.T, pre_grad, preferred_element_type=jnp.float32).astype(jnp.bfloat16)
    down_grad = jnp.dot(hidden.T, z_grad, preferred_element_type=jnp.float32).astype(jnp.bfloat16)
    return (x_grad, up_grad, down_grad)
```

```python
import functools
import math
import jax
import jax.numpy as jnp
from jax import lax
from jax.experimental import pallas as pl
from jax.experimental.pallas import tpu as pltpu
from jax.sharding import PartitionSpec as P

GELU_COEF = 0.044715
SQRT_TWO_PI = math.sqrt(2.0 / math.pi)
LAST = (((1,), (1,)), ((), ()))
FIRST = (((0,), (0,)), ((), ()))
SWAP = [(0, 1), (1, 0)]
F32 = jnp.float32
BF16 = jnp.bfloat16


def dot(a, b, dims=(((1,), (0,)), ((), ()))):
    return lax.dot_general(a, b, dims, preferred_element_type=F32)


def hidden_kernel(xo, xx, go, gx, wuo, wux, doa, dob, dxa, dxb, *rest):
    h_ref, dc_ref = rest[-2:]
    q = doa.shape[1]
    pre = dot(xo[...], wuo[...]) + dot(xx[...], wux[...])
    c = pre.astype(BF16).astype(F32)
    t = jnp.tanh(SQRT_TWO_PI * (c + GELU_COEF * c * c * c))
    h_ref[...] = (0.5 * c * (1.0 + t)).astype(BF16)
    slope = 0.5 * (1.0 + t) + 0.5 * c * (1.0 - t * t) * SQRT_TWO_PI * (1.0 + 3.0 * GELU_COEF * c * c)
    dh = dot(go[:, :q], doa[...], LAST) + dot(go[:, q:], dob[...], LAST)
    dh += dot(gx[:, :q], dxa[...], LAST) + dot(gx[:, q:], dxb[...], LAST)
    dc_ref[...] = (dh * slope).astype(BF16)


def hidden_call(rows, own, cross, half, wuo, wux, downs, after, bm=512, bn=512):
    (xo, xo_row), (go, go_row) = own
    (xx, xx_row), (gx, gx_row) = cross
    width = wuo.shape[1]
    depth = xo.shape[1]
    bm = min(bm, rows)

    def row_spec(row0):
        return pl.BlockSpec((bm, depth), lambda n, m, r=row0 // bm: (m + r, 0))

    up_spec = pl.BlockSpec((depth, bn), lambda n, m: (0, n))
    shift = half * (width // bn)
    down_spec = pl.BlockSpec((bn, downs[0].shape[1]), lambda n, m: (n + shift, 0))
    out_spec = pl.BlockSpec((bm, bn), lambda n, m: (m, n))
    out = jax.ShapeDtypeStruct((rows, width), BF16)
    extra = [pl.BlockSpec(memory_space=pl.ANY)] * len(after)
    return pl.pallas_call(
        hidden_kernel,
        grid=(width // bn, rows // bm),
        in_specs=[row_spec(xo_row), row_spec(xx_row), row_spec(go_row), row_spec(gx_row), up_spec, up_spec] + [down_spec] * 4 + extra,
        out_specs=[out_spec, out_spec],
        out_shape=[out, out],
        compiler_params=pltpu.CompilerParams(vmem_limit_bytes=56 * 2**20, dimension_semantics=("arbitrary", "arbitrary")),
        cost_estimate=pl.CostEstimate(flops=8 * rows * depth * width, bytes_accessed=4 * rows * depth * 2 + 4 * depth * width * 2, transcendentals=rows * width),
    )(xo, xx, go, gx, wuo, wux, *downs, *after)


def solution(mesh):
    row_spec = P(("dp", "cx", "cz"), "cy")
    up_spec = P("cy", ("cz", "cx"))
    down_spec = P("cz", ("cy", "cx"))
    up_out = P(("dp", "cy"), ("cz", "cx"))
    down_out = P(("dp", "cz"), ("cy", "cx"))

    def swap(v, axis):
        return lax.ppermute(v, axis, SWAP)

    def body(x, w_up, w_down, z):
        first = lax.axis_index("cx") == 0
        nt = x.shape[0]
        h = nt // 2
        q = w_down.shape[1]
        ff = w_up.shape[1]
        g = jnp.where(first, z, jnp.concatenate([z[:, q:], z[:, :q]], axis=1))
        wd = jnp.where(first, w_down, jnp.concatenate([w_down[ff:], w_down[:ff]], axis=0))

        x1, x2, g1, g2 = x[:h], x[h:], g[:h], g[h:]
        xy2 = swap(x2, "cz")
        gy2 = swap(g2, "cz")
        xy1 = swap(x1, "cz")
        gy1 = swap(g1, "cz")
        wu_x = swap(w_up, "cy")
        wd_x = swap(wd, "cy")
        xx1 = swap(x1, "cy")
        gx1 = swap(g1, "cy")
        xb2 = swap(xy2, "cy")
        gb2 = swap(gy2, "cy")
        xx2 = swap(x2, "cy")
        gx2 = swap(g2, "cy")
        wu_p = swap(w_up, "cx")
        wd_p = swap(jnp.concatenate([wd[ff:], wd[:ff]], axis=0), "cx")
        wux_p = swap(wu_x, "cx")
        wdx_p = swap(jnp.concatenate([wd_x[ff:], wd_x[:ff]], axis=0), "cx")
        xa1 = swap(xx1, "cz")
        ga1 = swap(gx1, "cz")

        downs = (wd, wd_p, wd_x, wdx_p)

        def unit(rows, own, cross, after):
            h0, c0 = hidden_call(rows, own, cross, 0, w_up, wu_x, downs, after)
            h1, c1 = hidden_call(rows, own, cross, 1, wu_p, wux_p, downs, (c0,))
            return (h0, h1), (c0, c1)

        def dx_part(dc):
            return dot(dc[0], w_up, LAST) + dot(dc[1], wu_p, LAST)

        h_o1, c_o1 = unit(h, ((x, 0), (g, 0)), ((xx1, 0), (gx1, 0)), ())
        h_a, c_a = unit(h, ((xy1, 0), (gy1, 0)), ((xa1, 0), (ga1, 0)), (c_o1[1],))
        dx_a = swap(dx_part(c_a), "cz")
        h_b, c_b = unit(h, ((xy2, 0), (gy2, 0)), ((xb2, 0), (gb2, 0)), (c_a[1],))
        dx_b = swap(dx_part(c_b), "cz")
        h_o2, c_o2 = unit(h, ((x, h), (g, h)), ((xx2, 0), (gx2, 0)), (c_b[1],))
        dx1 = (dx_part(c_o1) + dx_a).astype(BF16)
        dx2 = (dx_part(c_o2) + dx_b).astype(BF16)
        x_grad = jnp.concatenate([dx1, dx2], axis=0)

        xs = (x1, xy1, xy2, x2)
        gs = (g1, gy1, gy2, g2)
        hs = (h_o1, h_a, h_b, h_o2)
        cs = (c_o1, c_a, c_b, c_o2)

        def total(parts):
            return functools.reduce(lambda a, b: a + b, parts)

        up_send = total([dot(v, c[1], FIRST) for v, c in zip(xs, cs)])
        up_recv = swap(up_send, "cx")
        down_recv = []
        for half in range(2):
            send = total([dot(v[1 - half], w[:, q:], FIRST) for v, w in zip(hs, gs)])
            down_recv.append(swap(send, "cx"))
        up_grad = (total([dot(v, c[0], FIRST) for v, c in zip(xs, cs)]) + up_recv).astype(BF16)
        downs_out = [(total([dot(v[half], w[:, :q], FIRST) for v, w in zip(hs, gs)]) + down_recv[half]).astype(BF16) for half in range(2)]
        down_grad = jnp.where(first, jnp.concatenate(downs_out, axis=0), jnp.concatenate(downs_out[::-1], axis=0))
        return (x_grad, up_grad, down_grad)

    return jax.shard_map(body, mesh=mesh, in_specs=(row_spec, up_spec, down_spec, row_spec), out_specs=(row_spec, up_out, down_out), check_vma=False)
```
